32 devices in a mesh: row: 8 (over y, x, core), col: 4 (over z).
Axes of the slice: x: 2, y: 2, z: 4, core: 2. Of those that a mesh axis runs over, the one named last changes fastest.
Arguments:
- adjacency: int32 [2560, 80], P('row', 'col'), may hold values from -2147483648 to 2147483647, as said below
- relabel: int32 [2560], P(('row', 'col')), may hold values from 0 to 2559, each once
Outputs:
- clustering: float32 [2560], P(('row', 'col'))
- transitivity: float32 [], replicated
The draws below stay inside these ranges and needn't reach their ends.
Inputs may be any that keep to these rules, and one draw needn't show every extreme that they name: The unpacked adjacency is symmetric with a zero diagonal.
All inputs are finite; a program needn't handle non-finite values.
Results may differ from the reference program's by a relative error of at most 0.0003.
Values sent between devices are 32-bit elements.
No kernel may reach another device: no remote copies, remote signals or barrier semaphores. Data moves between devices by JAX's collectives and lax.ppermute only.
A program may use at most 128 MiB of HBM per device.

```python
import jax
import jax.numpy as jnp
from jax import lax

NV = 2560
N_ROW = 8


def draw_adjacency(key, part):
    first, second = jax.random.split(jax.random.fold_in(key, 23), 2)
    activity = jax.random.randint(first, (NV,), 1, 5)
    thresh = 1000 * activity[:, None] * activity[None, :]
    coins = jax.random.randint(second, (NV, NV), 0, 65536)
    keep = coins < thresh
    index = jnp.arange(NV)
    upper = keep & (index[None, :] > index[:, None])
    links = (upper | upper.T).astype(jnp.int32)
    bits = links.reshape(NV, NV // 32, 32)
    shifts = jnp.arange(32, dtype=jnp.int32)
    words = jnp.sum(lax.shift_left(bits, shifts[None, None, :]), axis=2)
    return words.astype(jnp.int32)


def setup_inputs(seed: int = 0) -> dict:
    key_list = jax.random.split(jax.random.key(seed), 3)
    return {
        "adjacency": draw_adjacency(jax.random.fold_in(key_list[2], 71), 0),
        "relabel": jax.random.permutation(key_list[1], NV).astype(jnp.int32),
    }


def unpack(words):
    shifts = jnp.arange(32, dtype=jnp.int32)
    bits = lax.shift_right_logical(words[:, :, None], shifts[None, None, :]) & 1
    return bits.reshape(words.shape[0], words.shape[1] * 32).astype(jnp.bfloat16)


def reference(adjacency, relabel):
    links = unpack(adjacency)
    block_rows = NV // N_ROW
    starts = jnp.arange(N_ROW, dtype=jnp.int32) * block_rows

    def one_block(offset):
        rows = lax.dynamic_slice_in_dim(links, offset.astype(jnp.int32), block_rows, 0)
        paths = jnp.dot(rows, links, preferred_element_type=jnp.float32)
        wide = rows.astype(jnp.float32)
        return jnp.sum(wide * paths, axis=1), jnp.sum(wide, axis=1)

    closed, degree = lax.map(one_block, starts)
    closed = closed.reshape(NV)
    degree = degree.reshape(NV)
    wedges = jnp.maximum(degree * (degree - 1.0), 1.0)
    ratio = closed / wedges
    clustering = jnp.take(ratio, relabel, axis=0)
    transitivity = jnp.sum(closed) / jnp.sum(wedges)
    return clustering, transitivity
```

```python
import jax
import jax.numpy as jnp
from jax import lax
from jax.experimental import pallas as pl
from jax.experimental.pallas import tpu as pltpu
from jax.sharding import PartitionSpec as P

BOTH = ("row", "col")
F8 = jnp.float8_e4m3fn
TILE = 256
LANE = 128
VMEM_BUDGET = 40 << 20


def unpack(words):
    shifts = jnp.arange(32, dtype=jnp.int32)
    bits = lax.shift_right_logical(words[:, :, None], shifts[None, None, :]) & 1
    return bits.reshape(words.shape[0], words.shape[1] * 32).astype(jnp.bfloat16)


def plain_body(adjacency, relabel):
    local = unpack(adjacency)
    row_block = unpack(lax.all_gather(adjacency, "col", axis=1, tiled=True))
    paths = jnp.dot(
        row_block,
        unpack(lax.all_gather(adjacency, "row", axis=0, tiled=True)),
        preferred_element_type=jnp.float32,
    )
    wide = local.astype(jnp.float32)
    partial_value = jnp.sum(wide * paths, axis=1)
    degree_part = jnp.sum(wide, axis=1)
    closed, degree = (
        lax.psum_scatter(partial_value, "col", scatter_dimension=0, tiled=True),
        lax.psum_scatter(degree_part, "col", scatter_dimension=0, tiled=True),
    )
    wedges = jnp.maximum(degree * (degree - 1.0), 1.0)
    everyone = lax.all_gather(closed / wedges, BOTH, axis=0, tiled=True)
    clustering = jnp.take(everyone, relabel, axis=0)
    sum_closed, sum_wedges = lax.psum((jnp.sum(closed), jnp.sum(wedges)), BOTH)
    return clustering, sum_closed / sum_wedges


def half_kernel(
    lists, here_ref, own_s, far_s, own_v, far_v, *refs, n_row, n_col, words, lanes, ask
):
    sources, (mine_ref, theirs_ref) = refs[:4], refs[4:6]
    blocks_ref, at_ref, e1_ref, e2_ref, sel_ref, raw_ref = refs[6:]
    half = lanes * n_row // 2
    n_words = words * n_col
    here = here_ref[0]
    side = here // (n_col * (n_row // 2))
    core = (here // n_col) % 2

    n_step = len(lists[0])
    for a, source in enumerate(sources):
        other = a // 2
        at_core = core ^ 1 if other else core
        for b in range(source.shape[0]):
            picks = b + (a % 2) * source.shape[0]
            flip = [sum(m for t, m in enumerate(ms) if picks >> t & 1) for ms in lists]
            flat = here ^ jnp.where(at_core == 0, flip[0], flip[1]) ^ (n_col * other)
            r, c = (flat // n_col) % (n_row // 2), (flat % n_col) ^ (side * (n_col // 2))
            blocks_ref[r * n_col + c] = source[b]
    for r in range(n_row // 2):
        for c in range(n_col):
            at_ref[c * words : (c + 1) * words, r * lanes : (r + 1) * lanes] = blocks_ref[
                r * n_col + c
            ]

    step = lax.broadcasted_iota(jnp.int32, (32, 1), 0)

    def bits_of(w, lo):
        row = jnp.broadcast_to(at_ref[w : w + 1, lo:half], (32, half - lo))
        return (lax.shift_right_logical(row, jnp.broadcast_to(step, row.shape)) & 1).astype(
            jnp.float32
        )

    for w in range(half // 32):
        lo = (w * 32) // TILE * TILE
        bits = bits_of(w, lo)
        col = lax.broadcasted_iota(jnp.int32, bits.shape, 1) + lo
        row = lax.broadcasted_iota(jnp.int32, bits.shape, 0) + w * 32
        bits = jnp.where(col > row, bits, 0.0)
        e1_ref[w * 32 : (w + 1) * 32, lo:half] = bits.astype(F8)
    for w in range(half // 32, n_words):
        at = w * 32 - half
        e2_ref[at : at + 32, :] = bits_of(w, 0).astype(F8)

    pad = sel_ref.shape[0] // 2
    for g, (sref, vref) in enumerate(((own_s, own_v), (far_s, far_v))):
        for v in range(ask):
            w = (sref[v] >> 5) + side * (n_words // 2)
            w = jnp.where(w >= n_words, w - n_words, w)
            raw_ref[g * pad + v : g * pad + v + 1, :] = at_ref[pl.ds(w, 1), :]
        for p in range(0, pad, LANE):
            live = min(LANE, ask - p)
            spots = jnp.zeros((1, LANE), jnp.int32)
            spots = jnp.pad(vref[:, p : p + live], ((0, 0), (0, LANE - live)), constant_values=-1)
            spots = jnp.broadcast_to(spots, (LANE, LANE)).T
            rows = slice(g * pad + p, g * pad + p + LANE)
            shift = spots & 31
            ok = spots >= 0
            for t in range(0, half, LANE):
                word = raw_ref[rows, t : t + LANE]
                bit = lax.shift_right_logical(word, shift) & 1
                e2_ref[half + g * pad + p : half + g * pad + p + LANE, t : t + LANE] = (
                    jnp.where(ok, bit, 0).astype(jnp.float32).astype(F8)
                )
                lane = lax.broadcasted_iota(jnp.int32, (LANE, LANE), 1) + t
                hit = spots - side * half == lane
                sel_ref[rows, t : t + LANE] = jnp.where(hit, 1.0, 0.0).astype(F8)

    def dot(a, b, dims=(((1,), (0,)), ((), ()))):
        return lax.dot_general(a, b, dims, preferred_element_type=jnp.float32)

    def fold(x):
        out = x[:, :LANE]
        for t in range(LANE, x.shape[1], LANE):
            out = out + x[:, t : t + LANE]
        return out

    total = jnp.zeros((8, LANE), jnp.float32)
    ask_closed = jnp.zeros((2 * pad, LANE), jnp.float32)
    ask_degree = jnp.zeros((2 * pad, LANE), jnp.float32)
    for k in range(0, half, TILE):
        for i in range(0, k + TILE, TILE):
            out = dot(e1_ref[i : i + TILE, i : k + TILE], e1_ref[i : k + TILE, k : k + TILE])
            out = fold(out * e1_ref[i : i + TILE, k : k + TILE].astype(jnp.float32))
            total = total + jnp.sum(out.reshape(-1, 8, LANE), axis=0)
        out = dot(e2_ref[:, : k + TILE], e1_ref[: k + TILE, k : k + TILE])
        mask = e2_ref[:, k : k + TILE].astype(jnp.float32)
        ask_degree = ask_degree + fold(mask[half:])
        out = fold(out * mask)
        total = total + jnp.sum(out[:half].reshape(-1, 8, LANE), axis=0)
        ask_closed = ask_closed + out[half:]

    lane_dims = (((1,), (1,)), ((), ()))
    walk = dot(e2_ref[:half, :], e2_ref[half:, :], lane_dims)
    link = dot(e2_ref[:half, :], sel_ref[...], lane_dims)
    cross = jnp.sum((walk * link).reshape(-1, 8, 2 * pad), axis=0)
    cross = jnp.sum(cross, axis=0, keepdims=True)

    degree = lax.population_count(at_ref[0:8, :])
    for w in range(8, n_words, 8):
        degree = degree + lax.population_count(at_ref[w : w + 8, :])
    degree = jnp.sum(degree.astype(jnp.float32), axis=0, keepdims=True)
    wedges = jnp.sum(jnp.maximum(degree * (degree - 1.0), 1.0))
    triangles = jnp.sum(total)
    for g, ref in enumerate((mine_ref, theirs_ref)):
        at = slice(g * pad, (g + 1) * pad)
        ref[0:1, :] = 2.0 * (jnp.sum(ask_closed[at].T, axis=0, keepdims=True) + cross[:, at])
        ref[1:2, :] = jnp.sum(ask_degree[at].T, axis=0, keepdims=True)
        ref[2:3, :] = jnp.full((1, pad), 6.0 * triangles, jnp.float32)
        ref[3:4, :] = jnp.full((1, pad), wedges, jnp.float32)


def swap(x, mask_of, size):
    return lax.ppermute(x, BOTH, [(i, i ^ mask_of(i)) for i in range(size)])


def half_body(adjacency, relabel, *, n_row, n_col):
    size = n_row * n_col
    lanes, words = adjacency.shape
    ask = relabel.shape[0]
    half = lanes * n_row // 2
    across = size // 2
    steps = [1 << t for t in reversed(range(n_col.bit_length() - 1))]
    steps += [n_col << t for t in range(1, n_row.bit_length() - 2)]
    lists = (tuple(steps), tuple(steps[:-2] + [steps[-1], steps[-2]]))

    def mask_at(t):
        return lambda i: lists[(i // n_col) % 2][t]

    far = swap(relabel, lambda i: across, size)
    have = adjacency.T[None]
    for t in range(len(steps) - 1):
        have = jnp.concatenate([have, swap(have, mask_at(t), size)], axis=0)
    last = swap(have, mask_at(len(steps) - 1), size)
    other = swap(have, lambda i: n_col, size)
    other_last = swap(last, lambda i: n_col, size)

    here = (lax.axis_index("row") * n_col + lax.axis_index("col")).astype(jnp.int32).reshape(1)
    pad = -(-ask // LANE) * LANE
    vmem = pl.BlockSpec(memory_space=pltpu.VMEM)
    smem = pl.BlockSpec(memory_space=pltpu.SMEM)

    def kernel(*refs):
        half_kernel(
            lists, *refs, n_row=n_row, n_col=n_col, words=words, lanes=lanes, ask=ask
        )

    mine, theirs = pl.pallas_call(
        kernel,
        in_specs=[smem, smem, smem, vmem, vmem] + [vmem] * 4,
        out_specs=[vmem, vmem],
        out_shape=[jax.ShapeDtypeStruct((8, pad), jnp.float32)] * 2,
        scratch_shapes=[
            pltpu.VMEM((n_row // 2 * n_col, words, lanes), jnp.int32),
            pltpu.VMEM((words * n_col, half), jnp.int32),
            pltpu.VMEM((half, half), F8),
            pltpu.VMEM((half + 2 * pad, half), F8),
            pltpu.VMEM((2 * pad, half), F8),
            pltpu.VMEM((2 * pad, half), jnp.int32),
        ],
        compiler_params=pltpu.CompilerParams(vmem_limit_bytes=VMEM_BUDGET),
        name="half_counts",
    )(here, relabel, far, relabel[None], far[None], have, last, other, other_last)

    got = mine + swap(theirs, lambda i: across, size)
    degree = got[1, :ask]
    clustering = got[0, :ask] / jnp.maximum(degree * (degree - 1.0), 1.0)
    return clustering, got[2, 0] / got[3, 0]


def fits(mesh, adjacency):
    n_row, n_col = mesh.shape["row"], mesh.shape["col"]
    nv = adjacency.shape[0]
    whole = n_row >= 8 and n_col >= 4 and n_row & (n_row - 1) == 0 and n_col & (n_col - 1) == 0
    return whole and nv % (2 * TILE) == 0 and 4 * nv * nv < 3 * VMEM_BUDGET


def solution(mesh):
    placed = (P("row", "col"), P(BOTH))

    def run(adjacency, relabel):
        body = plain_body
        if fits(mesh, adjacency):
            sizes = dict(n_row=mesh.shape["row"], n_col=mesh.shape["col"])
            body = lambda a, r: half_body(a, r, **sizes)
        return jax.shard_map(
            body, mesh=mesh, in_specs=placed, out_specs=(P(BOTH), P()), check_vma=False
        )(adjacency, relabel)

    return run
```

```python
import jax
import jax.numpy as jnp
from jax import lax
from jax.experimental import pallas as pl
from jax.experimental.pallas import tpu as pltpu
from jax.sharding import PartitionSpec as P

BOTH = ("row", "col")
F8 = jnp.float8_e4m3fn
TILE = 256
LANE = 128
VMEM_BUDGET = 40 << 20
SMALL = 2 << 20


def unpack(words):
    shifts = jnp.arange(32, dtype=jnp.int32)
    bits = lax.shift_right_logical(words[:, :, None], shifts[None, None, :]) & 1
    return bits.reshape(words.shape[0], words.shape[1] * 32).astype(jnp.bfloat16)


def plain_body(adjacency, relabel):
    local = unpack(adjacency)
    row_block = unpack(lax.all_gather(adjacency, "col", axis=1, tiled=True))
    paths = jnp.dot(
        row_block,
        unpack(lax.all_gather(adjacency, "row", axis=0, tiled=True)),
        preferred_element_type=jnp.float32,
    )
    wide = local.astype(jnp.float32)
    partial_value = jnp.sum(wide * paths, axis=1)
    degree_part = jnp.sum(wide, axis=1)
    closed, degree = (
        lax.psum_scatter(partial_value, "col", scatter_dimension=0, tiled=True),
        lax.psum_scatter(degree_part, "col", scatter_dimension=0, tiled=True),
    )
    wedges = jnp.maximum(degree * (degree - 1.0), 1.0)
    everyone = lax.all_gather(closed / wedges, BOTH, axis=0, tiled=True)
    clustering = jnp.take(everyone, relabel, axis=0)
    sum_closed, sum_wedges = lax.psum((jnp.sum(closed), jnp.sum(wedges)), BOTH)
    return clustering, sum_closed / sum_wedges


def half_kernel(
    masks, own_any, far_any, own_v, far_v, *refs, n_row, n_col, words, lanes, ask
):
    n_pair = 2 * len(masks)
    sources, (mine_ref, theirs_ref) = refs[:n_pair], refs[n_pair : n_pair + 2]
    blocks_ref, at_ref, e1_ref, e2_ref, sel_ref, raw_ref, own_s, far_s, sems = refs[n_pair + 2 :]
    half = lanes * n_row // 2
    n_words = words * n_col
    copies = [
        pltpu.make_async_copy(src, dst, sems.at[t])
        for t, (src, dst) in enumerate(((own_any, own_s), (far_any, far_s)))
    ]
    for copy in copies:
        copy.start()
    here = lax.axis_index("row") * n_col + lax.axis_index("col")
    side = here // (n_col * (n_row // 2))
    core = (here // n_col) % 2

    wide = 2 * lanes
    for t, source in enumerate(sources):
        pair = masks[t % len(masks)]
        mask = jnp.where((core ^ (t // len(masks))) == 0, pair[0], pair[1])
        flat = here ^ mask
        r, c = (flat // n_col) % (n_row // 2) // 2, (flat % n_col) ^ (side * (n_col // 2))
        if t < len(masks) or pair[0] != pair[1]:
            blocks_ref[r * n_col + c] = source[...]
    for r in range(n_row // 4):
        for c in range(n_col):
            for t in range(wide // LANE):
                at = r * wide + t * LANE
                at_ref[c * words : (c + 1) * words, at : at + LANE] = blocks_ref[
                    r * n_col + c, t * words : (t + 1) * words, :
                ]

    step = lax.broadcasted_iota(jnp.int32, (32, 1), 0)

    def bits_of(w, lo):
        row = jnp.broadcast_to(at_ref[w : w + 1, lo:half], (32, half - lo))
        return (lax.shift_right_logical(row, jnp.broadcast_to(step, row.shape)) & 1).astype(
            jnp.float32
        )

    for w in range(half // 32):
        lo = (w * 32) // TILE * TILE
        bits = bits_of(w, lo)
        col = lax.broadcasted_iota(jnp.int32, bits.shape, 1) + lo
        row = lax.broadcasted_iota(jnp.int32, bits.shape, 0) + w * 32
        bits = jnp.where(col > row, bits, 0.0)
        e1_ref[w * 32 : (w + 1) * 32, lo:half] = bits.astype(F8)
    for w in range(half // 32, n_words):
        at = w * 32 - half
        e2_ref[at : at + 32, :] = bits_of(w, 0).astype(F8)

    for copy in copies:
        copy.wait()
    pad = sel_ref.shape[0] // 2
    for g, (sref, vref) in enumerate(((own_s, own_v), (far_s, far_v))):
        for v in range(ask):
            w = (sref[v] >> 5) + side * (n_words // 2)
            w = jnp.where(w >= n_words, w - n_words, w)
            raw_ref[g * pad + v : g * pad + v + 1, :] = at_ref[pl.ds(w, 1), :]
        for p in range(0, pad, LANE):
            live = min(LANE, ask - p)
            spots = jnp.zeros((1, LANE), jnp.int32)
            spots = jnp.pad(vref[:, p : p + live], ((0, 0), (0, LANE - live)), constant_values=-1)
            spots = jnp.broadcast_to(spots, (LANE, LANE)).T
            rows = slice(g * pad + p, g * pad + p + LANE)
            shift = spots & 31
            ok = spots >= 0
            for t in range(0, half, LANE):
                word = raw_ref[rows, t : t + LANE]
                bit = lax.shift_right_logical(word, shift) & 1
                e2_ref[half + g * pad + p : half + g * pad + p + LANE, t : t + LANE] = (
                    jnp.where(ok, bit, 0).astype(jnp.float32).astype(F8)
                )
                lane = lax.broadcasted_iota(jnp.int32, (LANE, LANE), 1) + t
                hit = spots - side * half == lane
                sel_ref[rows, t : t + LANE] = jnp.where(hit, 1.0, 0.0).astype(F8)

    def dot(a, b, dims=(((1,), (0,)), ((), ()))):
        return lax.dot_general(a, b, dims, preferred_element_type=jnp.float32)

    def fold(x):
        out = x[:, :LANE]
        for t in range(LANE, x.shape[1], LANE):
            out = out + x[:, t : t + LANE]
        return out

    total = jnp.zeros((8, LANE), jnp.float32)
    ask_closed = jnp.zeros((2 * pad, LANE), jnp.float32)
    ask_degree = jnp.zeros((2 * pad, LANE), jnp.float32)
    for k in range(0, half, TILE):
        for i in range(0, k + TILE, TILE):
            out = dot(e1_ref[i : i + TILE, i : k + TILE], e1_ref[i : k + TILE, k : k + TILE])
            out = fold(out * e1_ref[i : i + TILE, k : k + TILE].astype(jnp.float32))
            total = total + jnp.sum(out.reshape(-1, 8, LANE), axis=0)
        out = dot(e2_ref[:, : k + TILE], e1_ref[: k + TILE, k : k + TILE])
        mask = e2_ref[:, k : k + TILE].astype(jnp.float32)
        ask_degree = ask_degree + fold(mask[half:])
        out = fold(out * mask)
        total = total + jnp.sum(out[:half].reshape(-1, 8, LANE), axis=0)
        ask_closed = ask_closed + out[half:]

    lane_dims = (((1,), (1,)), ((), ()))
    walk = dot(e2_ref[:half, :], e2_ref[half:, :], lane_dims)
    link = dot(e2_ref[:half, :], sel_ref[...], lane_dims)
    cross = jnp.sum((walk * link).reshape(-1, 8, 2 * pad), axis=0)
    cross = jnp.sum(cross, axis=0, keepdims=True)

    degree = lax.population_count(at_ref[0:8, :])
    for w in range(8, n_words, 8):
        degree = degree + lax.population_count(at_ref[w : w + 8, :])
    degree = jnp.sum(degree.astype(jnp.float32), axis=0, keepdims=True)
    wedges = jnp.sum(jnp.maximum(degree * (degree - 1.0), 1.0))
    triangles = jnp.sum(total)
    for g, ref in enumerate((mine_ref, theirs_ref)):
        at = slice(g * pad, (g + 1) * pad)
        ref[0:1, :] = 2.0 * (jnp.sum(ask_closed[at].T, axis=0, keepdims=True) + cross[:, at])
        ref[1:2, :] = jnp.sum(ask_degree[at].T, axis=0, keepdims=True)
        ref[2:3, :] = jnp.full((1, pad), 6.0 * triangles, jnp.float32)
        ref[3:4, :] = jnp.full((1, pad), wedges, jnp.float32)


def swap(x, mask_of, size):
    return lax.ppermute(x, BOTH, [(i, i ^ mask_of(i)) for i in range(size)])


def join_kernel(own_ref, got_ref, pair_ref):
    words, lanes = own_ref.shape
    own, got = own_ref[...], got_ref[...]
    first = lax.axis_index("row") % 2 == 0
    pair = jnp.concatenate([jnp.where(first, own, got), jnp.where(first, got, own)], axis=1)
    for t in range(2 * lanes // LANE):
        pair_ref[t * words : (t + 1) * words, :] = pair[:, t * LANE : (t + 1) * LANE]


def finish_kernel(mine_ref, got_ref, clustering_ref, transitivity_ref):
    both = mine_ref[...] + got_ref[...]
    degree = both[1:2, :]
    ratio = both[0:1, :] / jnp.maximum(degree * (degree - 1.0), 1.0)
    clustering_ref[...] = ratio[:, : clustering_ref.shape[1]]
    transitivity_ref[...] = both[2:3, :1] / both[3:4, :1]


def half_body(adjacency, relabel, *, n_row, n_col):
    size = n_row * n_col
    lanes, words = adjacency.shape
    ask = relabel.shape[0]
    half = lanes * n_row // 2
    across = size // 2
    top = size // 4
    inner = [(n_col << 1) * r + c for r in range(top // n_col // 2) for c in range(n_col)]
    masks = [(0, 0)] + [(m, m + top) for m in sorted(inner[1:], reverse=True)] + [(top, top)]
    vmem = pl.BlockSpec(memory_space=pltpu.VMEM)
    anywhere = pl.BlockSpec(memory_space=pl.ANY)

    def over(pair):
        return lambda i: pair[(i // n_col) % 2]

    own = adjacency.T
    other = swap(own, over((n_col, n_col)), size)
    pair = pl.pallas_call(
        join_kernel,
        in_specs=[vmem, vmem],
        out_specs=vmem,
        out_shape=jax.ShapeDtypeStruct((words * 2 * lanes // LANE, LANE), jnp.int32),
        compiler_params=pltpu.CompilerParams(vmem_limit_bytes=SMALL),
        name="join",
    )(own, other)
    pair, asked = lax.optimization_barrier((pair, relabel))
    got = [pair] + [swap(pair, over(m), size) for m in masks[1:]]
    far = swap(asked, lambda i: across, size)
    got[-2], far = lax.optimization_barrier((got[-2], far))
    crossed = [
        g if m[0] == m[1] else swap(g, over((n_col, n_col)), size) for g, m in zip(got, masks)
    ]

    pad = -(-ask // LANE) * LANE

    def kernel(*refs):
        half_kernel(
            masks, *refs, n_row=n_row, n_col=n_col, words=words, lanes=lanes, ask=ask
        )

    mine, theirs = pl.pallas_call(
        kernel,
        in_specs=[anywhere, anywhere, vmem, vmem] + [vmem] * (2 * len(masks)),
        out_specs=[vmem, vmem],
        out_shape=[jax.ShapeDtypeStruct((8, pad), jnp.float32)] * 2,
        scratch_shapes=[
            pltpu.VMEM((n_row // 4 * n_col, *pair.shape), jnp.int32),
            pltpu.VMEM((words * n_col, half), jnp.int32),
            pltpu.VMEM((half, half), F8),
            pltpu.VMEM((half + 2 * pad, half), F8),
            pltpu.VMEM((2 * pad, half), F8),
            pltpu.VMEM((2 * pad, half), jnp.int32),
            pltpu.SMEM((ask,), jnp.int32),
            pltpu.SMEM((ask,), jnp.int32),
            pltpu.SemaphoreType.DMA((2,)),
        ],
        compiler_params=pltpu.CompilerParams(vmem_limit_bytes=VMEM_BUDGET),
        name="half_counts",
    )(relabel, far, relabel[None], far[None], *got, *crossed)

    back = swap(theirs, lambda i: across, size)
    clustering, transitivity = pl.pallas_call(
        finish_kernel,
        in_specs=[vmem, vmem],
        out_specs=[vmem, vmem],
        out_shape=[
            jax.ShapeDtypeStruct((1, ask), jnp.float32),
            jax.ShapeDtypeStruct((1, 1), jnp.float32),
        ],
        compiler_params=pltpu.CompilerParams(vmem_limit_bytes=SMALL),
        name="finish",
    )(mine, back)
    return clustering[0], transitivity[0, 0]


def fits(mesh, adjacency):
    n_row, n_col = mesh.shape["row"], mesh.shape["col"]
    nv = adjacency.shape[0]
    whole = n_row >= 8 and n_col >= 4 and n_row & (n_row - 1) == 0 and n_col & (n_col - 1) == 0
    aligned = nv % (2 * TILE) == 0 and 2 * nv // n_row % LANE == 0
    return whole and aligned and 4 * nv * nv < 3 * VMEM_BUDGET


def solution(mesh):
    placed = (P("row", "col"), P(BOTH))

    def run(adjacency, relabel):
        body = plain_body
        if fits(mesh, adjacency):
            sizes = dict(n_row=mesh.shape["row"], n_col=mesh.shape["col"])
            body = lambda a, r: half_body(a, r, **sizes)
        return jax.shard_map(
            body, mesh=mesh, in_specs=placed, out_specs=(P(BOTH), P()), check_vma=False
        )(adjacency, relabel)

    return run
```
